32 devices in a mesh: row: 8 (over y, x, core), col: 4 (over z).
Axes of the slice: x: 2, y: 2, z: 4, core: 2. Of those that a mesh axis runs over, the one named last changes fastest.
Arguments:
- eigvectors: bfloat16 [14336, 256], P(('col', 'row')), may hold values from -0.046875 to 0.046875
- eigvalues: float32 [256], replicated, may hold values from -0.6 to 0.99
- degrees: float32 [14336], P(('col', 'row')), may hold values from 1 to 180
- sketch: bfloat16 [14336, 256], P(('col', 'row')), may hold values from -0.046875 to 0.046875
Outputs:
- embedding: float32 [14336, 256], P(('col', 'row'))
The draws below stay inside these ranges and needn't reach their ends.
All inputs are finite; a program needn't handle non-finite values.
Results may differ from the reference program's by a relative error of at most 0.0071.
Values may be sent and summed in bfloat16 or wider, within the bound.
A program may use at most 64 MiB of HBM per device.

```python
import math
import jax
import jax.numpy as jnp
from jax import lax

K = 256
S = 256
WINDOW = 10
N = 14336


def draw_degrees(key, part):
    first = jax.random.fold_in(key, 0)
    ramp = 1.0 + 2.0 * jnp.arange(N, dtype=jnp.float32) / (N - 1)
    base = jnp.exp(jax.random.uniform(first, (N,), jnp.float32, 0.0, math.log(20.0)))
    return base * ramp


def block_scale(key, dims, cuts, least, high):
    factor_of, own = 1.0, jax.random.fold_in(key, 6)
    for axis_at, blocks in cuts:
        heights = jnp.exp(jax.random.uniform(jax.random.fold_in(own, axis_at), (blocks,), jnp.float32, least / len(cuts), high / len(cuts)))
        factor_of = factor_of * jnp.repeat(heights, dims[axis_at] // blocks).reshape([-1 if axis == axis_at else 1 for axis in range(len(dims))])
    return factor_of


def normal_values(stream_key, dims, deviation, most, shards=(), kind=jnp.bfloat16):
    gain = block_scale(stream_key, dims, shards, -0.22, 0.18) if shards else 1.0
    drawn = jax.random.normal(stream_key, dims, jnp.float32) * deviation * gain
    return jnp.minimum(jnp.maximum(drawn, -most), most).astype(kind)


def setup_inputs(seed: int = 0) -> dict:
    key_of = jax.random.split(jax.random.key(seed), 5)
    eigvectors = normal_values(key_of[0], (N, K), N ** -0.5, 0.046875, ((0, 32),))
    eigvalues = jnp.clip(jax.random.uniform(key_of[1], (K,), jnp.float32, -0.6, 0.99), -0.6, 0.99)
    degrees = draw_degrees(jax.random.fold_in(key_of[4], 71), 0)
    sketch = normal_values(key_of[3], (N, S), N ** -0.5, 0.046875, ((0, 32),))
    return {"eigvectors": eigvectors, "eigvalues": eigvalues, "degrees": degrees, "sketch": sketch}


def spectrum(eigvalues):
    total = jnp.zeros_like(eigvalues)
    powers = jnp.ones_like(eigvalues)
    for counter in range(WINDOW):
        powers = powers * eigvalues
        total = total + powers
    return total / WINDOW

def reference(eigvectors, eigvalues, degrees, sketch):
    volume = jnp.sum(degrees)
    spectral = spectrum(eigvalues)
    right = (eigvectors.astype(jnp.float32) * lax.rsqrt(degrees)[:, None]).astype(jnp.bfloat16)
    left_rows = (right.astype(jnp.float32) * spectral[None, :]).astype(jnp.bfloat16)
    row_block = math.gcd(N, 1024)
    blocks = left_rows.reshape(N // row_block, row_block, K)

    def one_block(left_block):
        products = lax.dot_general(left_block, right, (((1,), (1,)), ((), ())), preferred_element_type=jnp.float32)
        matrix = volume * products
        log_values = jnp.log(jnp.maximum(matrix, 1.0)).astype(jnp.bfloat16)
        return jnp.dot(log_values, sketch, preferred_element_type=jnp.float32)
    return lax.map(one_block, blocks).reshape(N, S)
```

```python
import functools

import jax
import jax.numpy as jnp
from jax import lax
from jax.experimental import pallas as pl
from jax.experimental.pallas import tpu as pltpu
from jax.sharding import PartitionSpec as P

WINDOW = 10
MESH = pl.DeviceIdType.MESH


def spectrum(eigvalues):
    total = jnp.zeros_like(eigvalues)
    powers = jnp.ones_like(eigvalues)
    for counter in range(WINDOW):
        powers = powers * eigvalues
        total = total + powers
    return total / WINDOW


def kernel(nrow, ncol, right_ref, sketch_ref, deg_ref, eig_ref, out_ref,
           cright, csketch, rright, left, acc, sendbuf, recvbuf, dsum, drow, dpart, dcol,
           c_send, c_recv, z_send, z_recv, v_send, v_recv, w_send, w_recv, p_send, p_recv):
    r = lax.axis_index("row")
    c = lax.axis_index("col")
    chips = nrow // 2
    core = lax.rem(r, 2)
    chip = r // 2
    partner = (r + 1 - 2 * core, c)

    def row_peer(j):
        return (lax.rem(r + j, nrow), c)

    def col_peer(o):
        return (r, lax.rem(c + o, ncol))

    barrier = pltpu.get_barrier_semaphore()
    for j in range(1, nrow):
        pl.semaphore_signal(barrier, inc=1, device_id=row_peer(j), device_id_type=MESH)
    for o in range(1, ncol):
        pl.semaphore_signal(barrier, inc=1, device_id=col_peer(o), device_id_type=MESH)
    dsum[...] = jnp.full(dsum.shape, jnp.sum(deg_ref[...]), jnp.float32)
    pl.semaphore_wait(barrier, nrow + ncol - 2)

    def remote(src, dst, ssem, rsem, dev):
        return pltpu.make_async_remote_copy(
            src_ref=src, dst_ref=dst, send_sem=ssem, recv_sem=rsem,
            device_id=dev, device_id_type=MESH)

    bufs = (cright, csketch)
    owns = (right_ref, sketch_ref)
    started = []

    def start(copy):
        copy.start()
        started.append(copy)

    def c_copy(kind, src_slot, dst_slot, dev):
        src = owns[kind] if src_slot == 0 else bufs[kind].at[src_slot]
        return remote(src, bufs[kind].at[dst_slot], c_send.at[kind, dst_slot],
                      c_recv.at[kind, dst_slot], dev)

    def c_wait(kind, slot):
        c_copy(kind, 0, slot, partner).wait_recv()

    for j in range(1, nrow):
        start(remote(dsum, drow.at[j], v_send.at[j], v_recv.at[j], row_peer(j)))

    relay = chips == 4
    if relay:
        x_peer = chip + 1 - 2 * lax.rem(chip, 2)
        y_peer = lax.rem(chip + 2, 4)
        first = x_peer * (1 - core) + y_peer * core
        second = y_peer * (1 - core) + x_peer * core
        first = (first * 2 + core, c)
        second = (second * 2 + core, c)
        targets = [(1, first), (2, second)]
    else:
        targets = [(o, (lax.rem(chip + o, chips) * 2 + core, c)) for o in range(1, chips)]

    order = sorted(range(1, ncol), key=lambda o: -min(o, ncol - o))
    for kind in (0, 1):
        start(c_copy(kind, 0, 1, partner))
        for o, dev in targets:
            start(c_copy(kind, 0, 2 * o, dev))
        if kind == 0:
            for o in reversed(order):
                start(remote(right_ref, rright.at[o], z_send.at[o], z_recv.at[o], col_peer(o)))

    total = dsum[...]
    for j in range(1, nrow):
        remote(dsum, drow.at[j], v_send.at[j], v_recv.at[j], row_peer(j)).wait_recv()
        total = total + drow[j]
    dpart[...] = total
    spectral = spectrum(eig_ref[...])
    acc[...] = jnp.zeros_like(acc)
    left[0] = (right_ref[...].astype(jnp.float32) * spectral).astype(jnp.bfloat16)
    for o in range(1, ncol):
        start(remote(dpart, dcol.at[o], w_send.at[o], w_recv.at[o], col_peer(o)))
    for o in range(1, ncol):
        remote(dpart, dcol.at[o], w_send.at[o], w_recv.at[o], col_peer(o)).wait_recv()
        total = total + dcol[o]
    volume = total[0:1, 0:1]

    def tile(o, slot):
        cr = right_ref if slot == 0 else cright.at[slot]
        cs = sketch_ref if slot == 0 else csketch.at[slot]
        products = lax.dot_general(left[o], cr[...], (((1,), (1,)), ((), ())),
                                   preferred_element_type=jnp.float32)
        logs = jnp.log(jnp.maximum(volume * products, 1.0)).astype(jnp.bfloat16)
        acc[o] += jnp.dot(logs, cs[...], preferred_element_type=jnp.float32)

    def row_arrive(o):
        remote(right_ref, rright.at[o], z_send.at[o], z_recv.at[o], col_peer(o)).wait_recv()
        left[o] = (rright[o].astype(jnp.float32) * spectral).astype(jnp.bfloat16)

    def tiles(o, slots):
        for slot in slots:
            tile(o, slot)

    def many(lo, hi, slots):
        def step(o, carry):
            tiles(o, slots)
            return carry
        lax.fori_loop(lo, hi, step, 0)

    def c_arrive(kind, o):
        c_wait(kind, 2 * o)
        start(c_copy(kind, 2 * o, 2 * o + 1, partner))
        if relay and o == 1:
            start(c_copy(kind, 2, 6, second))

    tiles(0, [0])
    c_wait(0, 1)
    c_wait(1, 1)
    tiles(0, [1])
    c_arrive(0, 1)
    c_arrive(0, 2)
    for o in range(1, ncol):
        row_arrive(o)
    many(1, ncol, [0, 1])
    c_arrive(1, 1)
    c_arrive(1, 2)
    c_wait(0, 3)
    c_wait(1, 3)
    c_wait(0, 5)
    c_wait(1, 5)
    if relay:
        many(0, ncol, [2, 3, 4, 5])
        rest = [6, 7]
        c_arrive(0, 3)
        c_arrive(1, 3)
    else:
        many(0, ncol, [2, 3, 4, 5])
        rest = []
        for o in range(3, chips):
            c_arrive(0, o)
            c_arrive(1, o)
            rest += [2 * o, 2 * o + 1]
    for slot in rest[1::2]:
        c_wait(0, slot)
        c_wait(1, slot)

    def finish(o):
        if relay:
            tiles(o, rest)
        else:
            def step(slot, carry):
                products = lax.dot_general(left[o], cright[slot], (((1,), (1,)), ((), ())),
                                           preferred_element_type=jnp.float32)
                logs = jnp.log(jnp.maximum(volume * products, 1.0)).astype(jnp.bfloat16)
                acc[o] += jnp.dot(logs, csketch[slot], preferred_element_type=jnp.float32)
                return carry
            lax.fori_loop(6, 2 * chips, step, 0)

    def p_copy(o):
        return remote(sendbuf.at[o], recvbuf.at[o], p_send.at[o], p_recv.at[o], col_peer(o))

    for o in order:
        finish(o)
        sendbuf[ncol - o] = acc[o].astype(jnp.bfloat16)
        start(p_copy(ncol - o))
    finish(0)
    for o in reversed(order):
        p_copy(o).wait_recv()
        acc[0] += recvbuf[o].astype(jnp.float32)
    out_ref[...] = acc[0]
    for copy in started:
        copy.wait_send()


def local(nrow, ncol, eigvectors, eigvalues, degrees, sketch):
    rows, width = eigvectors.shape
    cols = sketch.shape[1]
    right = (eigvectors.astype(jnp.float32) * lax.rsqrt(degrees)[:, None]).astype(jnp.bfloat16)
    vmem = pl.BlockSpec(memory_space=pltpu.VMEM)
    dma = pltpu.SemaphoreType.DMA
    return pl.pallas_call(
        functools.partial(kernel, nrow, ncol),
        out_shape=jax.ShapeDtypeStruct((rows, cols), jnp.float32),
        in_specs=[vmem] * 4,
        out_specs=vmem,
        scratch_shapes=[
            pltpu.VMEM((nrow, rows, width), jnp.bfloat16),
            pltpu.VMEM((nrow, rows, cols), jnp.bfloat16),
            pltpu.VMEM((ncol, rows, width), jnp.bfloat16),
            pltpu.VMEM((ncol, rows, width), jnp.bfloat16),
            pltpu.VMEM((ncol, rows, cols), jnp.float32),
            pltpu.VMEM((ncol, rows, cols), jnp.bfloat16),
            pltpu.VMEM((ncol, rows, cols), jnp.bfloat16),
            pltpu.VMEM((8, 128), jnp.float32),
            pltpu.VMEM((nrow, 8, 128), jnp.float32),
            pltpu.VMEM((8, 128), jnp.float32),
            pltpu.VMEM((ncol, 8, 128), jnp.float32),
            dma((2, nrow)), dma((2, nrow)),
            dma((ncol,)), dma((ncol,)),
            dma((nrow,)), dma((nrow,)),
            dma((ncol,)), dma((ncol,)),
            dma((ncol,)), dma((ncol,)),
        ],
        compiler_params=pltpu.CompilerParams(
            collective_id=0, has_side_effects=True, vmem_limit_bytes=56 * 1024 * 1024),
    )(right, sketch, degrees.reshape(1, rows), eigvalues.reshape(1, width))


def solution(mesh):
    return jax.shard_map(
        functools.partial(local, mesh.shape["row"], mesh.shape["col"]),
        mesh=mesh,
        in_specs=(P(("col", "row"), None), P(), P(("col", "row")), P(("col", "row"), None)),
        out_specs=P(("col", "row"), None),
        check_vma=False,
    )
```

```python
import functools

import jax
import jax.numpy as jnp
from jax import lax
from jax.experimental import pallas as pl
from jax.experimental.pallas import tpu as pltpu
from jax.sharding import PartitionSpec as P

WINDOW = 10
MESH = pl.DeviceIdType.MESH


def spectrum(eigvalues):
    total = jnp.zeros_like(eigvalues)
    powers = jnp.ones_like(eigvalues)
    for counter in range(WINDOW):
        powers = powers * eigvalues
        total = total + powers
    return total / WINDOW


def kernel(nrow, ncol, right_ref, sketch_ref, deg_ref, eig_ref, out_ref,
           cright, csketch, rright, left, acc, sendbuf, recvbuf, dsum, dall,
           c_send, c_recv, z_send, z_recv, v_send, v_recv, p_send, p_recv):
    r = lax.axis_index("row")
    c = lax.axis_index("col")
    chips = nrow // 2
    core = lax.rem(r, 2)
    chip = r // 2
    partner = (r + 1 - 2 * core, c)

    rows = right_ref.shape[0]
    half = rows // 32 * 16
    everyone = nrow * ncol
    me = c * nrow + r

    def device(j):
        other = lax.rem(me + j, everyone)
        return (lax.rem(other, nrow), other // nrow)

    barrier = pltpu.get_barrier_semaphore()

    def greet(j, carry):
        pl.semaphore_signal(barrier, inc=1, device_id=device(j), device_id_type=MESH)
        return carry
    lax.fori_loop(1, everyone, greet, 0)
    dsum[...] = jnp.full(dsum.shape, jnp.sum(deg_ref[...]), jnp.float32)
    pl.semaphore_wait(barrier, everyone - 1)

    def remote(src, dst, ssem, rsem, dev):
        return pltpu.make_async_remote_copy(
            src_ref=src, dst_ref=dst, send_sem=ssem, recv_sem=rsem,
            device_id=dev, device_id_type=MESH)

    bufs = (cright, csketch)
    owns = (right_ref, sketch_ref)
    started = []

    def start(copy):
        copy.start()
        started.append(copy)

    def c_copy(kind, src_slot, dst_slot, dev):
        src = owns[kind] if src_slot == 0 else bufs[kind].at[src_slot]
        return remote(src, bufs[kind].at[dst_slot], c_send.at[kind, dst_slot],
                      c_recv.at[kind, dst_slot], dev)

    def c_wait(kind, slot):
        c_copy(kind, 0, slot, partner).wait_recv()

    def v_copy(j):
        return remote(dsum, dall.at[j], v_send.at[j], v_recv.at[j], device(j))

    def v_start(j, carry):
        v_copy(j).start()
        return carry
    lax.fori_loop(1, everyone, v_start, 0)
    dall[0] = dsum[...]

    relay = chips == 4
    if relay:
        x_peer = chip + 1 - 2 * lax.rem(chip, 2)
        y_peer = lax.rem(chip + 2, 4)
        first = x_peer * (1 - core) + y_peer * core
        second = y_peer * (1 - core) + x_peer * core
        first = (first * 2 + core, c)
        second = (second * 2 + core, c)
        targets = [(1, first), (2, second)]
    else:
        targets = [(o, (lax.rem(chip + o, chips) * 2 + core, c)) for o in range(1, chips)]

    line = ncol == 4
    if line:
        inner = lax.rem((c + 1) // 2, 2)
        way = 1 - 2 * (c // 2)
    else:
        inner, way = 1, 1

    def at(i):
        return lax.rem(c + i * way + ncol, ncol)

    def pick(end_i, inner_i):
        return at(end_i * (1 - inner) + inner_i * inner) if line else at(inner_i)

    def when_inner(fn):
        if line:
            pl.when(inner == 1)(fn)
        else:
            fn()

    def when_end(fn):
        if line:
            pl.when(inner == 0)(fn)

    halves = (pl.ds(0, half), pl.ds(half, rows - half))

    def z_copies(i):
        return [remote(right_ref.at[h], rright.at[c, h], z_send.at[n, i], z_recv.at[n, c], (r, at(i)))
                for n, h in enumerate(halves)]

    def z_half(n, src):
        h = halves[n]
        remote(right_ref.at[h], rright.at[src, h], z_send.at[n, 0], z_recv.at[n, src], (r, src)).wait_recv()

    def z_wait(src):
        z_half(0, src)
        z_half(1, src)

    def z_relay(n):
        far, h = at(2), halves[n]
        return remote(rright.at[far, h], rright.at[far, h], z_send.at[n, ncol], z_recv.at[n, far], (r, at(3)))

    def z_start(i):
        for copy in z_copies(i):
            copy.start()

    if line:
        z_start(2)
        z_start(1)
        when_inner(lambda: z_start(3))
    else:
        for i in range(1, ncol):
            z_start(i)
    for kind in (0, 1):
        start(c_copy(kind, 0, 1, partner))
        for o, dev in targets:
            start(c_copy(kind, 0, 2 * o, dev))

    spectral = spectrum(eig_ref[...])
    acc[...] = jnp.zeros_like(acc)
    cright[0] = right_ref[...]
    csketch[0] = sketch_ref[...]
    left[c] = (right_ref[...].astype(jnp.float32) * spectral).astype(jnp.bfloat16)

    def v_wait(j, carry):
        v_copy(j).wait_recv()
        return carry
    lax.fori_loop(1, everyone, v_wait, 0)
    volume = jnp.sum(dall[...], axis=0)[0:1, 0:1]

    def tiles(o, lo, hi):
        def step(slot, carry):
            products = lax.dot_general(left[o], cright[slot], (((1,), (1,)), ((), ())),
                                       preferred_element_type=jnp.float32)
            logs = jnp.log(jnp.maximum(volume * products, 1.0)).astype(jnp.bfloat16)
            acc[o] += jnp.dot(logs, csketch[slot], preferred_element_type=jnp.float32)
            return carry
        lax.fori_loop(lo, hi, step, 0)

    def row_scale(src):
        left[src] = (rright[src].astype(jnp.float32) * spectral).astype(jnp.bfloat16)

    def c_arrive(kind, o):
        c_wait(kind, 2 * o)
        start(c_copy(kind, 2 * o, 2 * o + 1, partner))
        if relay and o == 1:
            start(c_copy(kind, 2, 6, second))

    tiles(c, 0, 1)
    c_wait(0, 1)
    c_wait(1, 1)
    tiles(c, 1, 2)
    early = min(chips, 3)
    for o in range(1, early):
        c_arrive(0, o)
    def relay_row(n):
        z_half(n, at(2))
        z_relay(n).start()

    if line:
        when_inner(lambda: relay_row(0))
    first_row = pick(1, 3) if line else at(1)
    z_wait(first_row)
    row_scale(first_row)
    tiles(first_row, 0, 2)
    if line:
        when_inner(lambda: relay_row(1))
    for o in range(1, early):
        c_arrive(1, o)
    for o in range(1, early):
        c_wait(0, 2 * o + 1)
        c_wait(1, 2 * o + 1)
    tiles(c, 2, 2 * early)
    for o in range(early, chips):
        c_arrive(0, o)
    tiles(first_row, 2, 2 * early)
    if line:
        second_row, third_row = at(2), pick(3, 1)
        when_end(lambda: z_wait(second_row))
        row_scale(second_row)
        tiles(second_row, 0, 2 * early)
    for o in range(early, chips):
        c_arrive(1, o)
    if line:
        z_wait(third_row)
        row_scale(third_row)
        tiles(third_row, 0, 2 * early)
    else:
        for i in range(2, ncol):
            z_wait(at(i))
            row_scale(at(i))

        def other(i, carry):
            tiles(at(i), 0, 2 * early)
            return carry
        lax.fori_loop(2, ncol, other, 0)
    for o in range(early, chips):
        c_wait(0, 2 * o + 1)
        c_wait(1, 2 * o + 1)

    def p_copy(step, dst, slot):
        return remote(sendbuf.at[step], recvbuf.at[slot], p_send.at[step], p_recv.at[slot], (r, dst))

    def p_wait(src):
        p_copy(0, src, src).wait_recv()

    def finish(o):
        tiles(o, 2 * early, 2 * chips)

    if line:
        steps = [(pick(3, 1), at(1), ncol * (1 - inner) + c * inner), (pick(2, 3), pick(2, 3), c)]
        for step, (o, dst, slot) in enumerate(steps):
            finish(o)
            sendbuf[step] = acc[o].astype(jnp.bfloat16)
            start(p_copy(step, dst, slot))
        last = pick(1, 2)
        finish(last)

        def send_last():
            sendbuf[2] = acc[last].astype(jnp.bfloat16)
            p_copy(2, last, c).start()
        when_end(send_last)
        finish(c)

        def send_merged():
            p_copy(0, c, ncol).wait_recv()
            acc[last] += recvbuf[ncol].astype(jnp.float32)
            send_last()
        when_inner(send_merged)
        started.append(p_copy(2, last, c))
        p_wait(at(1))
        acc[c] += recvbuf[at(1)].astype(jnp.float32)

        def third():
            p_wait(at(3))
            acc[c] += recvbuf[at(3)].astype(jnp.float32)
        when_inner(third)
        p_wait(at(2))
        out_ref[...] = acc[c] + recvbuf[at(2)].astype(jnp.float32)

        def drain():
            for copy in z_copies(3) + [z_relay(0), z_relay(1)]:
                copy.wait_send()
        when_inner(drain)
    else:
        for i in range(1, ncol):
            finish(at(i))
            sendbuf[i] = acc[at(i)].astype(jnp.bfloat16)
            start(p_copy(i, at(i), c))
        finish(c)
        for i in range(1, ncol):
            p_wait(at(i))
            acc[c] += recvbuf[at(i)].astype(jnp.float32)
        out_ref[...] = acc[c]
    for i in range(1, 3 if line else ncol):
        started.extend(z_copies(i))
    for copy in started:
        copy.wait_send()

    def v_drain(j, carry):
        v_copy(j).wait_send()
        return carry
    lax.fori_loop(1, everyone, v_drain, 0)


def local(nrow, ncol, eigvectors, eigvalues, degrees, sketch):
    rows, width = eigvectors.shape
    cols = sketch.shape[1]
    right = (eigvectors.astype(jnp.float32) * lax.rsqrt(degrees)[:, None]).astype(jnp.bfloat16)
    vmem = pl.BlockSpec(memory_space=pltpu.VMEM)
    dma = pltpu.SemaphoreType.DMA
    return pl.pallas_call(
        functools.partial(kernel, nrow, ncol),
        out_shape=jax.ShapeDtypeStruct((rows, cols), jnp.float32),
        in_specs=[vmem] * 4,
        out_specs=vmem,
        scratch_shapes=[
            pltpu.VMEM((nrow, rows, width), jnp.bfloat16),
            pltpu.VMEM((nrow, rows, cols), jnp.bfloat16),
            pltpu.VMEM((ncol, rows, width), jnp.bfloat16),
            pltpu.VMEM((ncol, rows, width), jnp.bfloat16),
            pltpu.VMEM((ncol, rows, cols), jnp.float32),
            pltpu.VMEM((ncol, rows, cols), jnp.bfloat16),
            pltpu.VMEM((ncol + 1, rows, cols), jnp.bfloat16),
            pltpu.VMEM((1, 128), jnp.float32),
            pltpu.VMEM((nrow * ncol, 1, 128), jnp.float32),
            dma((2, nrow)), dma((2, nrow)),
            dma((2, ncol + 1)), dma((2, ncol)),
            dma((nrow * ncol,)), dma((nrow * ncol,)),
            dma((ncol,)), dma((ncol + 1,)),
        ],
        compiler_params=pltpu.CompilerParams(
            collective_id=0, has_side_effects=True, vmem_limit_bytes=56 * 1024 * 1024),
    )(right, sketch, degrees.reshape(1, rows), eigvalues.reshape(1, width))


def solution(mesh):
    return jax.shard_map(
        functools.partial(local, mesh.shape["row"], mesh.shape["col"]),
        mesh=mesh,
        in_specs=(P(("col", "row"), None), P(), P(("col", "row")), P(("col", "row"), None)),
        out_specs=P(("col", "row"), None),
        check_vma=False,
    )
```

```python
import functools

import jax
import jax.numpy as jnp
from jax import lax
from jax.experimental import pallas as pl
from jax.experimental.pallas import tpu as pltpu
from jax.sharding import PartitionSpec as P

WINDOW = 10
MESH = pl.DeviceIdType.MESH


def spectrum(eigvalues):
    total = jnp.zeros_like(eigvalues)
    powers = jnp.ones_like(eigvalues)
    for counter in range(WINDOW):
        powers = powers * eigvalues
        total = total + powers
    return total / WINDOW


def kernel(nrow, ncol, right_ref, sketch_ref, deg_ref, eig_ref, out_ref,
           cright, csketch, rright, left, acc, sendbuf, recvbuf, dsum, dall,
           c_send, c_recv, z_send, z_recv, v_send, v_recv, p_send, p_recv):
    r = lax.axis_index("row")
    c = lax.axis_index("col")
    chips = nrow // 2
    core = lax.rem(r, 2)
    chip = r // 2
    partner = (r + 1 - 2 * core, c)

    rows = right_ref.shape[0]
    half = rows // 32 * 16
    everyone = nrow * ncol
    me = c * nrow + r

    def device(j):
        other = lax.rem(me + j, everyone)
        return (lax.rem(other, nrow), other // nrow)

    barrier = pltpu.get_barrier_semaphore()

    def greet(j, carry):
        pl.semaphore_signal(barrier, inc=1, device_id=device(j), device_id_type=MESH)
        return carry
    lax.fori_loop(1, everyone, greet, 0)
    dsum[...] = jnp.full(dsum.shape, jnp.sum(deg_ref[...]), jnp.float32)
    pl.semaphore_wait(barrier, everyone - 1)

    def remote(src, dst, ssem, rsem, dev):
        return pltpu.make_async_remote_copy(
            src_ref=src, dst_ref=dst, send_sem=ssem, recv_sem=rsem,
            device_id=dev, device_id_type=MESH)

    bufs = (cright, csketch)
    owns = (right_ref, sketch_ref)
    started = []

    def start(copy):
        copy.start()
        started.append(copy)

    def c_copy(kind, src_slot, dst_slot, dev):
        src = owns[kind] if src_slot == 0 else bufs[kind].at[src_slot]
        return remote(src, bufs[kind].at[dst_slot], c_send.at[kind, dst_slot],
                      c_recv.at[kind, dst_slot], dev)

    def c_wait(kind, slot):
        c_copy(kind, 0, slot, partner).wait_recv()

    def v_copy(j):
        return remote(dsum, dall.at[j], v_send.at[j], v_recv.at[j], device(j))

    def v_start(j, carry):
        v_copy(j).start()
        return carry
    lax.fori_loop(1, everyone, v_start, 0)
    dall[0] = dsum[...]

    relay = chips == 4
    if relay:
        x_peer = chip + 1 - 2 * lax.rem(chip, 2)
        y_peer = lax.rem(chip + 2, 4)
        first = x_peer * (1 - core) + y_peer * core
        second = y_peer * (1 - core) + x_peer * core
        first = (first * 2 + core, c)
        second = (second * 2 + core, c)
        targets = [(1, first), (2, second)]
    else:
        targets = [(o, (lax.rem(chip + o, chips) * 2 + core, c)) for o in range(1, chips)]

    line = ncol == 4
    if line:
        inner = lax.rem((c + 1) // 2, 2)
        way = 1 - 2 * (c // 2)
    else:
        inner, way = 1, 1

    def at(i):
        return lax.rem(c + i * way + ncol, ncol)

    def pick(end_i, inner_i):
        return at(end_i * (1 - inner) + inner_i * inner) if line else at(inner_i)

    def when_inner(fn):
        if line:
            pl.when(inner == 1)(fn)
        else:
            fn()

    def when_end(fn):
        if line:
            pl.when(inner == 0)(fn)

    halves = (pl.ds(0, half), pl.ds(half, rows - half))

    def z_copies(i):
        return [remote(right_ref.at[h], rright.at[c, h], z_send.at[n, i], z_recv.at[n, c], (r, at(i)))
                for n, h in enumerate(halves)]

    def z_half(n, src):
        h = halves[n]
        remote(right_ref.at[h], rright.at[src, h], z_send.at[n, 0], z_recv.at[n, src], (r, src)).wait_recv()

    def z_wait(src):
        z_half(0, src)
        z_half(1, src)

    def z_relay(n):
        far, h = at(2), halves[n]
        return remote(rright.at[far, h], rright.at[far, h], z_send.at[n, ncol], z_recv.at[n, far], (r, at(3)))

    def z_start(i):
        for copy in z_copies(i):
            copy.start()

    if line:
        z_start(2)
        z_start(1)
        when_inner(lambda: z_start(3))
    else:
        for i in range(1, ncol):
            z_start(i)
    for kind in (0, 1):
        start(c_copy(kind, 0, 1, partner))
        for o, dev in targets:
            start(c_copy(kind, 0, 2 * o, dev))

    spectral = spectrum(eig_ref[...])
    acc[...] = jnp.zeros_like(acc)
    cright[0] = right_ref[...]
    csketch[0] = sketch_ref[...]
    left[c] = (right_ref[...].astype(jnp.float32) * spectral).astype(jnp.bfloat16)

    def v_wait(j, carry):
        v_copy(j).wait_recv()
        return carry
    lax.fori_loop(1, everyone, v_wait, 0)
    volume = jnp.sum(dall[...], axis=0)[0:1, 0:1]

    def tiles(o, lo, hi):
        def step(slot, carry):
            products = lax.dot_general(left[o], cright[slot], (((1,), (1,)), ((), ())),
                                       preferred_element_type=jnp.float32)
            logs = jnp.log(jnp.maximum(volume * products, 1.0)).astype(jnp.bfloat16)
            acc[o] += jnp.dot(logs, csketch[slot], preferred_element_type=jnp.float32)
            return carry
        lax.fori_loop(lo, hi, step, 0)

    def row_scale(src):
        left[src] = (rright[src].astype(jnp.float32) * spectral).astype(jnp.bfloat16)

    def c_arrive(kind, o):
        c_wait(kind, 2 * o)
        start(c_copy(kind, 2 * o, 2 * o + 1, partner))
        if relay and o == 1:
            start(c_copy(kind, 2, 6, second))

    tiles(c, 0, 1)
    c_wait(0, 1)
    c_wait(1, 1)
    tiles(c, 1, 2)
    early = min(chips, 3)
    for o in range(1, early):
        c_arrive(0, o)
    def relay_row(n):
        z_half(n, at(2))
        z_relay(n).start()

    if line:
        when_inner(lambda: relay_row(0))
    first_row = pick(1, 3) if line else at(1)
    z_wait(first_row)
    row_scale(first_row)
    tiles(first_row, 0, 2)
    if line:
        when_inner(lambda: relay_row(1))
    for o in range(1, early):
        c_arrive(1, o)
    for o in range(1, early):
        c_wait(0, 2 * o + 1)
        c_wait(1, 2 * o + 1)
    for o in range(early, chips):
        c_arrive(0, o)
    tiles(first_row, 2, 2 * early)
    if line:
        second_row, third_row = at(2), pick(3, 1)
        when_end(lambda: z_wait(second_row))
        row_scale(second_row)
    for o in range(early, chips):
        c_arrive(1, o)
    if line:
        z_wait(third_row)
        row_scale(third_row)
        tiles(third_row, 0, 2 * early)
    else:
        for i in range(2, ncol):
            z_wait(at(i))
            row_scale(at(i))

        def other(i, carry):
            tiles(at(i), 0, 2 * early)
            return carry
        lax.fori_loop(2, ncol, other, 0)
    for o in range(early, chips):
        c_wait(0, 2 * o + 1)
        c_wait(1, 2 * o + 1)

    def p_copy(step, dst, slot):
        return remote(sendbuf.at[step], recvbuf.at[slot], p_send.at[step], p_recv.at[slot], (r, dst))

    def p_wait(src):
        p_copy(0, src, src).wait_recv()

    def finish(o):
        tiles(o, 2 * early, 2 * chips)

    if line:
        steps = [(pick(3, 1), at(1), ncol * (1 - inner) + c * inner), (pick(2, 3), pick(2, 3), c)]
        for step, (o, dst, slot) in enumerate(steps):
            finish(o)
            sendbuf[step] = acc[o].astype(jnp.bfloat16)
            start(p_copy(step, dst, slot))
            if step == 0:
                tiles(second_row, 0, 2 * early)
        last = pick(1, 2)
        finish(last)

        def send_last():
            sendbuf[2] = acc[last].astype(jnp.bfloat16)
            p_copy(2, last, c).start()
        when_end(send_last)
        tiles(c, 2, 2 * chips)

        def send_merged():
            p_copy(0, c, ncol).wait_recv()
            acc[last] += recvbuf[ncol].astype(jnp.float32)
            send_last()
        when_inner(send_merged)
        started.append(p_copy(2, last, c))
        p_wait(at(1))
        acc[c] += recvbuf[at(1)].astype(jnp.float32)

        def third():
            p_wait(at(3))
            acc[c] += recvbuf[at(3)].astype(jnp.float32)
        when_inner(third)
        p_wait(at(2))
        out_ref[...] = acc[c] + recvbuf[at(2)].astype(jnp.float32)

        def drain():
            for copy in z_copies(3) + [z_relay(0), z_relay(1)]:
                copy.wait_send()
        when_inner(drain)
    else:
        for i in range(1, ncol):
            finish(at(i))
            sendbuf[i] = acc[at(i)].astype(jnp.bfloat16)
            start(p_copy(i, at(i), c))
        tiles(c, 2, 2 * chips)
        for i in range(1, ncol):
            p_wait(at(i))
            acc[c] += recvbuf[at(i)].astype(jnp.float32)
        out_ref[...] = acc[c]
    for i in range(1, 3 if line else ncol):
        started.extend(z_copies(i))
    for copy in started:
        copy.wait_send()

    def v_drain(j, carry):
        v_copy(j).wait_send()
        return carry
    lax.fori_loop(1, everyone, v_drain, 0)


def local(nrow, ncol, eigvectors, eigvalues, degrees, sketch):
    rows, width = eigvectors.shape
    cols = sketch.shape[1]
    right = (eigvectors.astype(jnp.float32) * lax.rsqrt(degrees)[:, None]).astype(jnp.bfloat16)
    vmem = pl.BlockSpec(memory_space=pltpu.VMEM)
    dma = pltpu.SemaphoreType.DMA
    return pl.pallas_call(
        functools.partial(kernel, nrow, ncol),
        out_shape=jax.ShapeDtypeStruct((rows, cols), jnp.float32),
        in_specs=[vmem] * 4,
        out_specs=vmem,
        scratch_shapes=[
            pltpu.VMEM((nrow, rows, width), jnp.bfloat16),
            pltpu.VMEM((nrow, rows, cols), jnp.bfloat16),
            pltpu.VMEM((ncol, rows, width), jnp.bfloat16),
            pltpu.VMEM((ncol, rows, width), jnp.bfloat16),
            pltpu.VMEM((ncol, rows, cols), jnp.float32),
            pltpu.VMEM((ncol, rows, cols), jnp.bfloat16),
            pltpu.VMEM((ncol + 1, rows, cols), jnp.bfloat16),
            pltpu.VMEM((1, 128), jnp.float32),
            pltpu.VMEM((nrow * ncol, 1, 128), jnp.float32),
            dma((2, nrow)), dma((2, nrow)),
            dma((2, ncol + 1)), dma((2, ncol)),
            dma((nrow * ncol,)), dma((nrow * ncol,)),
            dma((ncol,)), dma((ncol + 1,)),
        ],
        compiler_params=pltpu.CompilerParams(
            collective_id=0, has_side_effects=True, vmem_limit_bytes=56 * 1024 * 1024),
    )(right, sketch, degrees.reshape(1, rows), eigvalues.reshape(1, width))


def solution(mesh):
    return jax.shard_map(
        functools.partial(local, mesh.shape["row"], mesh.shape["col"]),
        mesh=mesh,
        in_specs=(P(("col", "row"), None), P(), P(("col", "row")), P(("col", "row"), None)),
        out_specs=P(("col", "row"), None),
        check_vma=False,
    )
```
